32 devices in a mesh: blk: 4 (over y, x), grp: 8 (over z, core).
Axes of the slice: x: 2, y: 2, z: 4, core: 2. Of those that a mesh axis runs over, the one named last changes fastest.
Arguments:
- queries: bfloat16 [32, 32, 128], P('blk', 'grp'), may hold values from -3 to 3
- token_counts: int32 [32], P('blk'), may hold values from 8 to 32
- pages: bfloat16 [32, 1024, 128], P(('blk', 'grp')), may hold values from -6 to 6
- patch_counts: int32 [32], P(('blk', 'grp')), may hold values from 512 to 1024
- labels: int32 [32, 32], P(None, ('blk', 'grp')), may hold values 0 or 1
Outputs:
- query_grad: float32 [32, 32, 128], P('blk', 'grp')
- page_grad: float32 [32, 1024, 128], P(('blk', 'grp'))
- page_loss: float32 [32], P(('blk', 'grp'))
The draws below stay inside these ranges and needn't reach their ends.
All inputs are finite; a program needn't handle non-finite values. No bound on the sum of `labels` on one device may be relied on, other than what follows from the above.
Results may differ from the reference program's by a relative error of at most 0.018.
Values may be sent and summed in bfloat16 or wider, within the bound.
A program may use at most 64 MiB of HBM per device.

```python
import jax
import jax.numpy as jnp
from jax import lax

EMBED_DIM = 128
QUERY_TOKENS = 32
PAGE_PATCHES = 1024
QUERY_COUNT = 32
PAGE_COUNT = 32


def page_values(key):
    base = jax.random.normal(jax.random.fold_in(key, 11), (PAGE_COUNT, PAGE_PATCHES, EMBED_DIM), jnp.float32)
    values = base
    return jnp.clip(values, -6.0, 6.0)


def draw_pages(key, part):
    return page_values(key).astype(jnp.bfloat16)


def draw_queries(key, part):
    base = 0.088 * jax.random.normal(jax.random.fold_in(key, 21), (QUERY_COUNT, QUERY_TOKENS, EMBED_DIM), jnp.float32)
    return jnp.clip(base, -3.0, 3.0).astype(jnp.bfloat16)


def set_ends(result, key, least, top_value):
    dims = result.shape
    place = [jax.random.randint(jax.random.fold_in(key, axis), (), 0, dims[axis]) for axis in range(len(dims))]
    result = result.at[tuple(place)].set(least)
    longest = dims.index(max(dims))
    place[longest] = (place[longest] + 1) % dims[longest]
    return result.at[tuple(place)].set(top_value)


def setup_inputs(seed: int = 0) -> dict:
    key_list = jax.random.split(jax.random.key(seed), 6)
    queries = draw_queries(jax.random.fold_in(key_list[5], 71), 0)
    token_counts = set_ends(jax.random.randint(key_list[1], (QUERY_COUNT,), QUERY_TOKENS // 4, QUERY_TOKENS + 1), jax.random.fold_in(key_list[1], 1), QUERY_TOKENS // 4, QUERY_TOKENS).astype(jnp.int32)
    pages = draw_pages(jax.random.fold_in(key_list[5], 71), 0)
    patch_counts = set_ends(jax.random.randint(key_list[3], (PAGE_COUNT,), PAGE_PATCHES // 2, PAGE_PATCHES + 1), jax.random.fold_in(key_list[3], 1), PAGE_PATCHES // 2, PAGE_PATCHES).astype(jnp.int32)
    labels = set_ends((jax.random.randint(key_list[4], (QUERY_COUNT, PAGE_COUNT), 0, 32) < 1).astype(jnp.int32), jax.random.fold_in(key_list[4], 1), 0, 1)
    return {"queries": queries, "token_counts": token_counts, "pages": pages, "patch_counts": patch_counts, "labels": labels}


align_sharpness = 4.0
logit_scale = 2.0
logit_bias = -5.0


def align(query_rows, counts, page_rows, patch_count, label_column):
    query_number = counts.shape[0]
    token_slots = query_rows.shape[0] // query_number
    scores = jnp.dot(query_rows, page_rows.T, preferred_element_type=jnp.float32)
    patch_mask = jnp.arange(page_rows.shape[0]) < patch_count
    logits = jnp.where(patch_mask[None, :], align_sharpness * scores, -jnp.inf)
    row_max = jnp.max(logits, axis=1, keepdims=True)
    exponent = jnp.exp(logits - row_max)
    weights = exponent / jnp.sum(exponent, axis=1, keepdims=True)
    token_score = jnp.sum(weights * scores, axis=1)
    token_mask = jnp.arange(token_slots)[None, :] < counts[:, None]
    count_float = counts.astype(jnp.float32)
    pair_score = jnp.sum(jnp.where(token_mask, token_score.reshape(query_number, token_slots), jnp.float32(0.0)), axis=1) / count_float
    label_sign = 2.0 * label_column.astype(jnp.float32) - 1.0
    pair_logit = logit_scale * pair_score + logit_bias
    loss_sum = jnp.sum(jax.nn.softplus(-label_sign * pair_logit))
    score_grad = -label_sign * logit_scale * jax.nn.sigmoid(-label_sign * pair_logit)
    token_grad = jnp.where(token_mask, (score_grad / count_float)[:, None], jnp.float32(0.0)).reshape(-1)
    scores_grad = (token_grad[:, None] * weights * (1.0 + align_sharpness * (scores - token_score[:, None]))).astype(jnp.bfloat16)
    query_term = jnp.dot(scores_grad, page_rows, preferred_element_type=jnp.float32)
    page_term = jnp.dot(scores_grad.T, query_rows, preferred_element_type=jnp.float32)
    return query_term, page_term, loss_sum


def reference(queries, token_counts, pages, patch_counts, labels):
    query_rows = queries.reshape(-1, queries.shape[2])

    def scan_step(query_total, entries):
        page_rows, patch_count, label_column = entries
        query_term, page_term, loss_sum = align(query_rows, token_counts, page_rows, patch_count, label_column)
        return query_total + query_term, (page_term, loss_sum)

    initial = jnp.zeros(query_rows.shape, jnp.float32)
    query_total, (page_grads, losses) = lax.scan(scan_step, initial, (pages, patch_counts, labels.T))
    page_loss = losses / jnp.float32(queries.shape[0])
    return query_total.reshape(queries.shape), page_grads, page_loss
```

```python
import functools
import math

import jax
import jax.numpy as jnp
from jax import lax
from jax.experimental import pallas as pl
from jax.experimental.pallas import tpu as pltpu
from jax.sharding import PartitionSpec as P

align_sharpness = 4.0
logit_scale = 2.0
logit_bias = -5.0
masked = -1e30
exp2_scale = align_sharpness * math.log2(math.e)
MESH = pl.DeviceIdType.MESH
patch_tile = 128


def partner(position, step, size):
    if size & (size - 1):
        return lax.rem(position + step, size)
    result = 0
    bit = 1
    while bit < size:
        here = lax.rem(position // bit, 2)
        flip = (step // bit) % 2
        result = result + (1 - here if flip else here) * bit
        bit *= 2
    return result


def source(position, step, size):
    if size & (size - 1):
        return lax.rem(position + size - step, size)
    return partner(position, step, size)


def fold(value):
    return value.reshape(-1, 8, value.shape[1])


def kernel(
    blocks, groups, block_queries, slice_tokens,
    query_ref, count_ref, page_ref, patch_count_ref, label_ref,
    query_grad_ref, page_grad_ref, loss_ref,
    held, count_rows, bias, scores, exponents, grads, own_term,
    part_send, part_recv, sum_send, sum_recv,
    column_send, column_recv, row_send, row_recv, count_send, count_recv,
    part_send_sem, part_recv_sem, sum_send_sem, sum_recv_sem,
):
    blk = lax.axis_index("blk")
    grp = lax.axis_index("grp")
    patches, width = page_ref.shape
    rows = block_queries * slice_tokens
    block_rows = rows * groups
    total_queries = blocks * block_queries
    tiles = [pl.ds(start, patch_tile) for start in range(0, patches, patch_tile)]

    barrier = pltpu.get_barrier_semaphore()
    for step in range(1, groups):
        pl.semaphore_signal(
            barrier, inc=1, device_id=(blk, partner(grp, step, groups)), device_id_type=MESH
        )
    for step in range(1, blocks):
        pl.semaphore_signal(
            barrier, inc=1, device_id=(partner(blk, step, blocks), grp), device_id_type=MESH
        )

    lane = lax.broadcasted_iota(jnp.int32, (1, block_rows), 1)
    query_row = lax.rem(lane // slice_tokens, block_queries)
    token_row = lane // rows * slice_tokens + lax.rem(lane, slice_tokens)
    counts = jnp.zeros((1, block_rows), jnp.float32)
    for index in range(block_queries):
        counts = jnp.where(query_row == index, count_ref[index].astype(jnp.float32), counts)
    count_rows[blk] = counts
    held[blk, grp] = query_ref[...]

    pl.semaphore_wait(barrier, groups - 1 + blocks - 1)

    def remote(src, dst, send, recv, device):
        pltpu.make_async_remote_copy(
            src_ref=src, dst_ref=dst, send_sem=send, recv_sem=recv,
            device_id=device, device_id_type=MESH,
        ).start()

    def settle(ref, sem):
        pltpu.make_async_copy(ref, ref, sem).wait()

    for step in range(groups - 1, 0, -1):
        remote(
            query_ref, held.at[blk, grp], column_send, column_recv.at[grp],
            (blk, partner(grp, step, groups)),
        )
    for step in range(1, blocks):
        other = partner(blk, step, blocks)
        remote(query_ref, held.at[blk, grp], row_send, row_recv.at[blk], (other, grp))
        remote(count_rows.at[blk], count_rows.at[blk], count_send, count_recv.at[blk], (other, grp))

    patch_count = patch_count_ref[0]
    for index, tile in enumerate(tiles):
        patch = index * patch_tile + lax.broadcasted_iota(jnp.int32, (patch_tile, width), 0)
        bias[tile, :] = jnp.where(patch < patch_count, 0.0, masked)
    same_query = (
        lax.rem(lax.broadcasted_iota(jnp.int32, (block_rows, block_rows), 0) // slice_tokens, block_queries)
        == lax.rem(lax.broadcasted_iota(jnp.int32, (block_rows, block_rows), 1) // slice_tokens, block_queries)
    )
    same_query = jnp.where(same_query, 1.0, 0.0).astype(jnp.bfloat16)

    for step in range(1, groups):
        origin = source(grp, step, groups)
        settle(held.at[blk, origin], column_recv.at[origin])
        for hop in range(1, blocks):
            remote(
                held.at[blk, origin], held.at[blk, origin], row_send, row_recv.at[blk],
                (partner(blk, hop, blocks), grp),
            )

    def block_terms(origin):
        query_rows = held[origin].reshape(block_rows, width)
        row_max = None
        for tile in tiles:
            tile_scores = lax.dot_general(
                page_ref[tile, :], query_rows, (((1,), (1,)), ((), ())),
                preferred_element_type=jnp.float32,
            )
            tile_bias = bias[tile, :]
            tile_scores = tile_scores + jnp.concatenate([tile_bias] * (block_rows // width), axis=1)
            scores[tile, :] = tile_scores
            tile_max = jnp.max(fold(tile_scores), axis=0)
            row_max = tile_max if row_max is None else jnp.maximum(row_max, tile_max)
        row_max = jnp.max(row_max, axis=0, keepdims=True)
        total = jnp.zeros((8, block_rows), jnp.float32)
        moment = jnp.zeros((8, block_rows), jnp.float32)
        for tile in tiles:
            shifted = scores[tile, :] - row_max
            exponent = jnp.exp2(shifted * exp2_scale)
            scores[tile, :] = shifted
            exponents[tile, :] = exponent
            total = total + jnp.sum(fold(exponent), axis=0)
            moment = moment + jnp.sum(fold(exponent * shifted), axis=0)
        total = jnp.sum(total, axis=0, keepdims=True)
        shifted_score = jnp.sum(moment, axis=0, keepdims=True) / total
        token_score = shifted_score + row_max

        count_row = count_rows[origin]
        live = token_row.astype(jnp.float32) < count_row
        remaining = jnp.where(live, token_score, 0.0)
        pieces = []
        for _ in range(3):
            piece = remaining.astype(jnp.bfloat16)
            pieces.append(piece)
            remaining = remaining - piece.astype(jnp.float32)
        pair_sum = sum(
            jnp.dot(
                jnp.broadcast_to(piece, (16, block_rows)), same_query,
                preferred_element_type=jnp.float32,
            )
            for piece in pieces
        )[0:1]
        pair_score = pair_sum / count_row
        label_row = jnp.zeros((1, block_rows), jnp.float32)
        for index in range(block_queries):
            label = label_ref[0, origin * block_queries + index].astype(jnp.float32)
            label_row = jnp.where(query_row == index, label, label_row)
        label_sign = 2.0 * label_row - 1.0
        signed = -label_sign * (logit_scale * pair_score + logit_bias)
        decay = jnp.exp(-jnp.abs(signed))
        softplus = jnp.maximum(signed, 0.0) + jnp.log1p(decay)
        sigmoid = jnp.where(signed >= 0.0, 1.0, decay) / (1.0 + decay)
        loss_row = jnp.where(token_row == 0, softplus, 0.0)
        token_grad = jnp.where(live, -label_sign * logit_scale * sigmoid / count_row, 0.0) / total
        slope = token_grad * align_sharpness
        offset = token_grad * (1.0 - align_sharpness * shifted_score)
        for tile in tiles:
            tile_grad = exponents[tile, :] * (offset + slope * scores[tile, :])
            grads[origin, tile, :] = tile_grad.astype(jnp.bfloat16)
        query_term = lax.dot_general(
            grads[origin], page_ref[...], (((0,), (0,)), ((), ())),
            preferred_element_type=jnp.float32,
        )
        return query_term, loss_row

    own, loss_row = block_terms(blk)
    own_term[...] = own.reshape(groups, rows, width)

    for step in range(1, blocks):
        origin = source(blk, step, blocks)
        settle(held.at[origin], row_recv.at[origin])
        settle(count_rows.at[origin], count_recv.at[origin])
        query_term, loss_term = block_terms(origin)
        loss_row = loss_row + loss_term
        part_send[origin] = query_term.astype(jnp.bfloat16).reshape(groups, rows, width)
        remote(
            part_send.at[origin], part_recv.at[blk], part_send_sem, part_recv_sem.at[blk],
            (origin, grp),
        )

    def page_term(tile):
        result = jnp.dot(
            grads[0, tile, :], held[0].reshape(block_rows, width), preferred_element_type=jnp.float32
        )
        for index in range(1, blocks):
            result = result + jnp.dot(
                grads[index, tile, :], held[index].reshape(block_rows, width),
                preferred_element_type=jnp.float32,
            )
        page_grad_ref[tile, :] = result

    half = len(tiles) // 2
    for tile in tiles[:half]:
        page_term(tile)

    block_sum = own_term[...]
    for step in range(1, blocks):
        origin = source(blk, step, blocks)
        settle(part_recv.at[origin], part_recv_sem.at[origin])
        block_sum = block_sum + part_recv[origin].astype(jnp.float32)
    own_term[...] = block_sum
    sum_send[...] = block_sum.astype(jnp.bfloat16)
    for step in range(groups - 1, 0, -1):
        target = partner(grp, step, groups)
        remote(
            sum_send.at[target], sum_recv.at[step - 1], sum_send_sem, sum_recv_sem, (blk, target)
        )
    for tile in tiles[half:]:
        page_term(tile)
    loss_ref[0] = jnp.sum(loss_row) / jnp.float32(total_queries)

    settle(sum_recv, sum_recv_sem)
    result = own_term[grp]
    for step in range(1, groups):
        result = result + sum_recv[step - 1].astype(jnp.float32)
    query_grad_ref[...] = result

    settle(held.at[0, pl.ds(0, groups - 1)], column_send)
    settle(held.at[pl.ds(0, blocks - 1)], row_send)
    settle(count_rows.at[pl.ds(0, blocks - 1)], count_send)
    settle(part_send.at[pl.ds(0, blocks - 1)], part_send_sem)
    settle(sum_send.at[pl.ds(0, groups - 1)], sum_send_sem)


def local(queries, token_counts, pages, patch_counts, labels):
    blocks = lax.axis_size("blk")
    groups = lax.axis_size("grp")
    block_queries, slice_tokens, width = queries.shape
    patches = pages.shape[1]
    rows = block_queries * slice_tokens
    block_rows = rows * groups
    vmem = pl.BlockSpec(memory_space=pltpu.VMEM)
    smem = pl.BlockSpec(memory_space=pltpu.SMEM)
    dma = pltpu.SemaphoreType.DMA
    query_grad, page_grad, page_loss = pl.pallas_call(
        functools.partial(kernel, blocks, groups, block_queries, slice_tokens),
        out_shape=(
            jax.ShapeDtypeStruct((rows, width), jnp.float32),
            jax.ShapeDtypeStruct((patches, width), jnp.float32),
            jax.ShapeDtypeStruct((1,), jnp.float32),
        ),
        in_specs=[vmem, smem, vmem, smem, smem],
        out_specs=(vmem, vmem, smem),
        scratch_shapes=[
            pltpu.VMEM((blocks, groups, rows, width), jnp.bfloat16),
            pltpu.VMEM((blocks, 1, block_rows), jnp.float32),
            pltpu.VMEM((patches, width), jnp.float32),
            pltpu.VMEM((patches, block_rows), jnp.float32),
            pltpu.VMEM((patches, block_rows), jnp.float32),
            pltpu.VMEM((blocks, patches, block_rows), jnp.bfloat16),
            pltpu.VMEM((groups, rows, width), jnp.float32),
            pltpu.VMEM((blocks, groups, rows, width), jnp.bfloat16),
            pltpu.VMEM((blocks, groups, rows, width), jnp.bfloat16),
            pltpu.VMEM((groups, rows, width), jnp.bfloat16),
            pltpu.VMEM((groups - 1, rows, width), jnp.bfloat16),
            dma, dma((groups,)), dma, dma((blocks,)), dma, dma((blocks,)),
            dma, dma((blocks,)), dma, dma,
        ],
        compiler_params=pltpu.CompilerParams(
            collective_id=0, has_side_effects=True, vmem_limit_bytes=60 * 1024 * 1024
        ),
        name="late_interaction",
    )(queries.reshape(rows, width), token_counts, pages[0], patch_counts, labels.T)
    return query_grad.reshape(queries.shape), page_grad[None], page_loss


def solution(mesh):
    in_specs = (
        P("blk", "grp", None),
        P("blk"),
        P(("blk", "grp"), None, None),
        P(("blk", "grp")),
        P(None, ("blk", "grp")),
    )
    out_specs = (P("blk", "grp", None), P(("blk", "grp"), None, None), P(("blk", "grp")))
    return jax.shard_map(local, mesh=mesh, in_specs=in_specs, out_specs=out_specs, check_vma=False)
```

```python
import functools
import math

import jax
import jax.numpy as jnp
from jax import lax
from jax.experimental import pallas as pl
from jax.experimental.pallas import tpu as pltpu
from jax.sharding import PartitionSpec as P

align_sharpness = 4.0
logit_scale = 2.0
logit_bias = -5.0
masked = -1e30
exp2_scale = align_sharpness * math.log2(math.e)
MESH = pl.DeviceIdType.MESH
patch_tile = 128


def partner(position, step, size):
    if size & (size - 1):
        return lax.rem(position + step, size)
    result = 0
    bit = 1
    while bit < size:
        here = lax.rem(position // bit, 2)
        flip = (step // bit) % 2
        result = result + (1 - here if flip else here) * bit
        bit *= 2
    return result


def source(position, step, size):
    if size & (size - 1):
        return lax.rem(position + size - step, size)
    return partner(position, step, size)


def fold(value):
    return value.reshape(-1, 8, value.shape[1])


def kernel(
    blocks, groups, block_queries, slice_tokens,
    query_in, count_in, page_in, patch_count_in, label_in,
    query_grad_ref, page_grad_ref, loss_ref,
    query_ref, count_ref, page_ref, patch_count_ref, label_ref,
    held, count_rows, bias, scores, exponents, grads, own_term,
    part_send, part_recv, sum_send, sum_recv,
    column_send, column_recv, row_send, row_recv, count_send, count_recv,
    part_send_sem, part_recv_sem, sum_send_sem, sum_recv_sem, load_sem,
):
    blk = lax.axis_index("blk")
    grp = lax.axis_index("grp")
    patches, width = page_ref.shape
    rows = block_queries * slice_tokens
    block_rows = rows * groups
    total_queries = blocks * block_queries
    tiles = [pl.ds(start, patch_tile) for start in range(0, patches, patch_tile)]

    barrier = pltpu.get_barrier_semaphore()
    for step in range(1, groups):
        pl.semaphore_signal(
            barrier, inc=1, device_id=(blk, partner(grp, step, groups)), device_id_type=MESH
        )
    for step in range(blocks - 1, 0, -1):
        pl.semaphore_signal(
            barrier, inc=1, device_id=(partner(blk, step, blocks), grp), device_id_type=MESH
        )

    loads = [
        pltpu.make_async_copy(src, dst, load_sem.at[index])
        for index, (src, dst) in enumerate((
            (query_in, query_ref), (count_in, count_ref), (page_in, page_ref),
            (patch_count_in, patch_count_ref), (label_in, label_ref),
        ))
    ]
    for load in loads:
        load.start()

    lane = lax.broadcasted_iota(jnp.int32, (1, block_rows), 1)
    query_row = lax.rem(lane // slice_tokens, block_queries)
    token_row = lane // rows * slice_tokens + lax.rem(lane, slice_tokens)
    loads[0].wait()
    loads[1].wait()
    counts = jnp.zeros((1, block_rows), jnp.float32)
    for index in range(block_queries):
        counts = jnp.where(query_row == index, count_ref[index].astype(jnp.float32), counts)
    count_rows[blk] = counts
    held[blk, grp] = query_ref[...]

    pl.semaphore_wait(barrier, groups - 1 + blocks - 1)

    def remote(src, dst, send, recv, device):
        pltpu.make_async_remote_copy(
            src_ref=src, dst_ref=dst, send_sem=send, recv_sem=recv,
            device_id=device, device_id_type=MESH,
        ).start()

    def settle(ref, sem):
        pltpu.make_async_copy(ref, ref, sem).wait()

    for step in range(groups - 1, 0, -1):
        remote(
            query_ref, held.at[blk, grp], column_send, column_recv.at[grp],
            (blk, partner(grp, step, groups)),
        )
    for step in range(blocks - 1, 0, -1):
        other = partner(blk, step, blocks)
        remote(query_ref, held.at[blk, grp], row_send, row_recv.at[blk], (other, grp))
        remote(count_rows.at[blk], count_rows.at[blk], count_send, count_recv.at[blk], (other, grp))

    for load in loads[2:]:
        load.wait()
    patch_count = patch_count_ref[0]
    for index, tile in enumerate(tiles):
        patch = index * patch_tile + lax.broadcasted_iota(jnp.int32, (patch_tile, width), 0)
        bias[tile, :] = jnp.where(patch < patch_count, 0.0, masked)
    same_query = (
        lax.rem(lax.broadcasted_iota(jnp.int32, (block_rows, block_rows), 0) // slice_tokens, block_queries)
        == lax.rem(lax.broadcasted_iota(jnp.int32, (block_rows, block_rows), 1) // slice_tokens, block_queries)
    )
    same_query = jnp.where(same_query, 1.0, 0.0).astype(jnp.bfloat16)

    for step in range(1, groups):
        origin = source(grp, step, groups)
        settle(held.at[blk, origin], column_recv.at[origin])
        for hop in range(blocks - 1, 0, -1):
            remote(
                held.at[blk, origin], held.at[blk, origin], row_send, row_recv.at[blk],
                (partner(blk, hop, blocks), grp),
            )

    def block_terms(origin):
        query_rows = held[origin].reshape(block_rows, width)
        row_max = None
        for tile in tiles:
            tile_scores = lax.dot_general(
                page_ref[tile, :], query_rows, (((1,), (1,)), ((), ())),
                preferred_element_type=jnp.float32,
            )
            tile_bias = bias[tile, :]
            tile_scores = tile_scores + jnp.concatenate([tile_bias] * (block_rows // width), axis=1)
            scores[tile, :] = tile_scores
            tile_max = jnp.max(fold(tile_scores), axis=0)
            row_max = tile_max if row_max is None else jnp.maximum(row_max, tile_max)
        row_max = jnp.max(row_max, axis=0, keepdims=True)
        total = jnp.zeros((8, block_rows), jnp.float32)
        moment = jnp.zeros((8, block_rows), jnp.float32)
        for tile in tiles:
            shifted = scores[tile, :] - row_max
            exponent = jnp.exp2(shifted * exp2_scale)
            scores[tile, :] = shifted
            exponents[tile, :] = exponent
            total = total + jnp.sum(fold(exponent), axis=0)
            moment = moment + jnp.sum(fold(exponent * shifted), axis=0)
        total = jnp.sum(total, axis=0, keepdims=True)
        shifted_score = jnp.sum(moment, axis=0, keepdims=True) / total
        token_score = shifted_score + row_max

        count_row = count_rows[origin]
        live = token_row.astype(jnp.float32) < count_row
        remaining = jnp.where(live, token_score, 0.0)
        pieces = []
        for _ in range(3):
            piece = remaining.astype(jnp.bfloat16)
            pieces.append(piece)
            remaining = remaining - piece.astype(jnp.float32)
        pair_sum = sum(
            jnp.dot(
                jnp.broadcast_to(piece, (16, block_rows)), same_query,
                preferred_element_type=jnp.float32,
            )
            for piece in pieces
        )[0:1]
        pair_score = pair_sum / count_row
        label_row = jnp.zeros((1, block_rows), jnp.float32)
        for index in range(block_queries):
            label = label_ref[0, origin * block_queries + index].astype(jnp.float32)
            label_row = jnp.where(query_row == index, label, label_row)
        label_sign = 2.0 * label_row - 1.0
        signed = -label_sign * (logit_scale * pair_score + logit_bias)
        decay = jnp.exp(-jnp.abs(signed))
        softplus = jnp.maximum(signed, 0.0) + jnp.log1p(decay)
        sigmoid = jnp.where(signed >= 0.0, 1.0, decay) / (1.0 + decay)
        loss_row = jnp.where(token_row == 0, softplus, 0.0)
        token_grad = jnp.where(live, -label_sign * logit_scale * sigmoid / count_row, 0.0) / total
        slope = token_grad * align_sharpness
        offset = token_grad * (1.0 - align_sharpness * shifted_score)
        for tile in tiles:
            tile_grad = exponents[tile, :] * (offset + slope * scores[tile, :])
            grads[origin, tile, :] = tile_grad.astype(jnp.bfloat16)
        query_term = lax.dot_general(
            grads[origin], page_ref[...], (((0,), (0,)), ((), ())),
            preferred_element_type=jnp.float32,
        )
        return query_term, loss_row

    own, loss_row = block_terms(blk)
    own_term[...] = own.reshape(groups, rows, width)

    for step in range(blocks - 1, 0, -1):
        origin = source(blk, step, blocks)
        settle(held.at[origin], row_recv.at[origin])
        settle(count_rows.at[origin], count_recv.at[origin])
        query_term, loss_term = block_terms(origin)
        loss_row = loss_row + loss_term
        part_send[origin] = query_term.astype(jnp.bfloat16).reshape(groups, rows, width)
        remote(
            part_send.at[origin], part_recv.at[blk], part_send_sem, part_recv_sem.at[blk],
            (origin, grp),
        )

    def page_term(tile):
        result = jnp.dot(
            grads[0, tile, :], held[0].reshape(block_rows, width), preferred_element_type=jnp.float32
        )
        for index in range(1, blocks):
            result = result + jnp.dot(
                grads[index, tile, :], held[index].reshape(block_rows, width),
                preferred_element_type=jnp.float32,
            )
        page_grad_ref[tile, :] = result

    half = len(tiles) // 2
    for tile in tiles[:half]:
        page_term(tile)

    block_sum = own_term[...]
    for step in range(blocks - 1, 0, -1):
        origin = source(blk, step, blocks)
        settle(part_recv.at[origin], part_recv_sem.at[origin])
        block_sum = block_sum + part_recv[origin].astype(jnp.float32)
    own_term[...] = block_sum
    sum_send[...] = block_sum.astype(jnp.bfloat16)
    for step in range(groups - 1, 0, -1):
        target = partner(grp, step, groups)
        remote(
            sum_send.at[target], sum_recv.at[step - 1], sum_send_sem, sum_recv_sem, (blk, target)
        )
    for tile in tiles[half:]:
        page_term(tile)
    loss_ref[0] = jnp.sum(loss_row) / jnp.float32(total_queries)

    settle(sum_recv, sum_recv_sem)
    result = own_term[grp]
    for step in range(1, groups):
        result = result + sum_recv[step - 1].astype(jnp.float32)
    query_grad_ref[...] = result

    settle(held.at[0, pl.ds(0, groups - 1)], column_send)
    settle(held.at[pl.ds(0, blocks - 1)], row_send)
    settle(count_rows.at[pl.ds(0, blocks - 1)], count_send)
    settle(part_send.at[pl.ds(0, blocks - 1)], part_send_sem)
    settle(sum_send.at[pl.ds(0, groups - 1)], sum_send_sem)


def write_out(query_grad_in, page_grad_in, loss_in, query_grad_ref, page_grad_ref, loss_ref, sems):
    copies = [
        pltpu.make_async_copy(page_grad_in, page_grad_ref, sems.at[0]),
        pltpu.make_async_copy(query_grad_in, query_grad_ref, sems.at[1]),
        pltpu.make_async_copy(loss_in, loss_ref, sems.at[2]),
    ]
    for copy in copies:
        copy.start()
    for copy in copies:
        copy.wait()


def local(queries, token_counts, pages, patch_counts, labels):
    blocks = lax.axis_size("blk")
    groups = lax.axis_size("grp")
    block_queries, slice_tokens, width = queries.shape
    patches = pages.shape[1]
    rows = block_queries * slice_tokens
    block_rows = rows * groups
    vmem = pl.BlockSpec(memory_space=pltpu.VMEM)
    smem = pl.BlockSpec(memory_space=pltpu.SMEM)
    anywhere = pl.BlockSpec(memory_space=pl.ANY)
    dma = pltpu.SemaphoreType.DMA
    query_grad, page_grad, page_loss = pl.pallas_call(
        functools.partial(kernel, blocks, groups, block_queries, slice_tokens),
        out_shape=(
            pltpu.VMEM((rows, width), jnp.float32),
            pltpu.VMEM((patches, width), jnp.float32),
            pltpu.SMEM((1,), jnp.float32),
        ),
        in_specs=[anywhere] * 5,
        out_specs=(vmem, vmem, smem),
        scratch_shapes=[
            pltpu.VMEM((rows, width), jnp.bfloat16),
            pltpu.SMEM(token_counts.shape, jnp.int32),
            pltpu.VMEM((patches, width), jnp.bfloat16),
            pltpu.SMEM((1,), jnp.int32),
            pltpu.SMEM((1, labels.shape[0]), jnp.int32),
            pltpu.VMEM((blocks, groups, rows, width), jnp.bfloat16),
            pltpu.VMEM((blocks, 1, block_rows), jnp.float32),
            pltpu.VMEM((patches, width), jnp.float32),
            pltpu.VMEM((patches, block_rows), jnp.float32),
            pltpu.VMEM((patches, block_rows), jnp.float32),
            pltpu.VMEM((blocks, patches, block_rows), jnp.bfloat16),
            pltpu.VMEM((groups, rows, width), jnp.float32),
            pltpu.VMEM((blocks, groups, rows, width), jnp.bfloat16),
            pltpu.VMEM((blocks, groups, rows, width), jnp.bfloat16),
            pltpu.VMEM((groups, rows, width), jnp.bfloat16),
            pltpu.VMEM((groups - 1, rows, width), jnp.bfloat16),
            dma, dma((groups,)), dma, dma((blocks,)), dma, dma((blocks,)),
            dma, dma((blocks,)), dma, dma, dma((5,)),
        ],
        compiler_params=pltpu.CompilerParams(
            collective_id=0, has_side_effects=True, vmem_limit_bytes=60 * 1024 * 1024
        ),
        name="late_interaction",
    )(queries.reshape(rows, width), token_counts, pages[0], patch_counts, labels.T)
    query_grad, page_grad, page_loss = pl.pallas_call(
        write_out,
        out_shape=(
            jax.ShapeDtypeStruct((rows, width), jnp.float32),
            jax.ShapeDtypeStruct((patches, width), jnp.float32),
            jax.ShapeDtypeStruct((1,), jnp.float32),
        ),
        in_specs=[anywhere] * 3,
        out_specs=(anywhere,) * 3,
        scratch_shapes=[dma((3,))],
        compiler_params=pltpu.CompilerParams(vmem_limit_bytes=1024 * 1024),
        name="write_out",
    )(query_grad, page_grad, page_loss)
    return query_grad.reshape(queries.shape), page_grad[None], page_loss


def solution(mesh):
    in_specs = (
        P("blk", "grp", None),
        P("blk"),
        P(("blk", "grp"), None, None),
        P(("blk", "grp")),
        P(None, ("blk", "grp")),
    )
    out_specs = (P("blk", "grp", None), P(("blk", "grp"), None, None), P(("blk", "grp")))
    return jax.shard_map(local, mesh=mesh, in_specs=in_specs, out_specs=out_specs, check_vma=False)
```

```python
import functools
import math

import jax
import jax.numpy as jnp
from jax import lax
from jax.experimental import pallas as pl
from jax.experimental.pallas import tpu as pltpu
from jax.sharding import PartitionSpec as P

align_sharpness = 4.0
logit_scale = 2.0
logit_bias = -5.0
masked = -1e30
exp2_scale = align_sharpness * math.log2(math.e)
MESH = pl.DeviceIdType.MESH
patch_tile = 128


def partner(position, step, size):
    if size & (size - 1):
        return lax.rem(position + step, size)
    result = 0
    bit = 1
    while bit < size:
        here = lax.rem(position // bit, 2)
        flip = (step // bit) % 2
        result = result + (1 - here if flip else here) * bit
        bit *= 2
    return result


def source(position, step, size):
    if size & (size - 1):
        return lax.rem(position + size - step, size)
    return partner(position, step, size)


def fold(value):
    return value.reshape(-1, 8, value.shape[1])


def kernel(
    blocks, groups, block_queries, slice_tokens,
    query_in, count_in, page_in, patch_count_in, label_in,
    query_grad_ref, page_grad_ref, loss_ref,
    query_ref, count_ref, page_ref, patch_count_ref, label_ref,
    held, count_rows, bias, scores, exponents, grads, own_term,
    part_send, part_recv, sum_send, sum_recv,
    column_send, column_recv, row_send, row_recv, count_send, count_recv,
    part_send_sem, part_recv_sem, sum_send_sem, sum_recv_sem, load_sem,
):
    blk = lax.axis_index("blk")
    grp = lax.axis_index("grp")
    patches, width = page_ref.shape
    rows = block_queries * slice_tokens
    block_rows = rows * groups
    total_queries = blocks * block_queries
    tiles = [pl.ds(start, patch_tile) for start in range(0, patches, patch_tile)]

    barrier = pltpu.get_barrier_semaphore()
    for step in range(1, groups):
        pl.semaphore_signal(
            barrier, inc=1, device_id=(blk, partner(grp, step, groups)), device_id_type=MESH
        )
    for step in range(blocks - 1, 0, -1):
        pl.semaphore_signal(
            barrier, inc=1, device_id=(partner(blk, step, blocks), grp), device_id_type=MESH
        )

    loads = [
        pltpu.make_async_copy(src, dst, load_sem.at[index])
        for index, (src, dst) in enumerate((
            (query_in, query_ref), (count_in, count_ref), (page_in, page_ref),
            (patch_count_in, patch_count_ref), (label_in, label_ref),
        ))
    ]
    for load in loads:
        load.start()

    lane = lax.broadcasted_iota(jnp.int32, (1, block_rows), 1)
    query_row = lax.rem(lane // slice_tokens, block_queries)
    token_row = lane // rows * slice_tokens + lax.rem(lane, slice_tokens)
    loads[0].wait()
    loads[1].wait()
    counts = jnp.zeros((1, block_rows), jnp.float32)
    for index in range(block_queries):
        counts = jnp.where(query_row == index, count_ref[index].astype(jnp.float32), counts)
    count_rows[blk] = counts
    held[blk, grp] = query_ref[...]

    pl.semaphore_wait(barrier, groups - 1 + blocks - 1)

    def remote(src, dst, send, recv, device):
        pltpu.make_async_remote_copy(
            src_ref=src, dst_ref=dst, send_sem=send, recv_sem=recv,
            device_id=device, device_id_type=MESH,
        ).start()

    def settle(ref, sem):
        pltpu.make_async_copy(ref, ref, sem).wait()

    for step in range(groups - 1, 0, -1):
        remote(
            query_ref, held.at[blk, grp], column_send, column_recv.at[grp],
            (blk, partner(grp, step, groups)),
        )
    for step in range(blocks - 1, 0, -1):
        other = partner(blk, step, blocks)
        remote(query_ref, held.at[blk, grp], row_send, row_recv.at[blk], (other, grp))
        remote(count_rows.at[blk], count_rows.at[blk], count_send, count_recv.at[blk], (other, grp))

    for load in loads[2:]:
        load.wait()
    patch_count = patch_count_ref[0]
    for index, tile in enumerate(tiles):
        patch = index * patch_tile + lax.broadcasted_iota(jnp.int32, (patch_tile, width), 0)
        bias[tile, :] = jnp.where(patch < patch_count, 0.0, masked)
    same_query = (
        lax.rem(lax.broadcasted_iota(jnp.int32, (block_rows, block_rows), 0) // slice_tokens, block_queries)
        == lax.rem(lax.broadcasted_iota(jnp.int32, (block_rows, block_rows), 1) // slice_tokens, block_queries)
    )
    same_query = jnp.where(same_query, 1.0, 0.0).astype(jnp.bfloat16)

    for step in range(1, groups):
        origin = source(grp, step, groups)
        settle(held.at[blk, origin], column_recv.at[origin])
        for hop in range(blocks - 1, 0, -1):
            remote(
                held.at[blk, origin], held.at[blk, origin], row_send, row_recv.at[blk],
                (partner(blk, hop, blocks), grp),
            )

    def block_terms(origin):
        query_rows = held[origin].reshape(block_rows, width)
        row_max = None
        for tile in tiles:
            tile_scores = lax.dot_general(
                page_ref[tile, :], query_rows, (((1,), (1,)), ((), ())),
                preferred_element_type=jnp.float32,
            )
            tile_bias = bias[tile, :]
            tile_scores = tile_scores + jnp.concatenate([tile_bias] * (block_rows // width), axis=1)
            scores[tile, :] = tile_scores
            tile_max = jnp.max(fold(tile_scores), axis=0)
            row_max = tile_max if row_max is None else jnp.maximum(row_max, tile_max)
        row_max = jnp.max(row_max, axis=0, keepdims=True)
        total = jnp.zeros((8, block_rows), jnp.float32)
        moment = jnp.zeros((8, block_rows), jnp.float32)
        for tile in tiles:
            shifted = scores[tile, :] - row_max
            exponent = jnp.exp2(shifted * exp2_scale)
            scores[tile, :] = shifted
            exponents[tile, :] = exponent
            total = total + jnp.sum(fold(exponent), axis=0)
            moment = moment + jnp.sum(fold(exponent * shifted), axis=0)
        total = jnp.sum(total, axis=0, keepdims=True)
        shifted_score = jnp.sum(moment, axis=0, keepdims=True) / total
        token_score = shifted_score + row_max

        count_row = count_rows[origin]
        live = token_row.astype(jnp.float32) < count_row
        remaining = jnp.where(live, token_score, 0.0)
        sublane = lax.broadcasted_iota(jnp.int32, (16, block_rows), 0)
        pieces = jnp.zeros((16, block_rows), jnp.float32)
        for index in range(3):
            piece = remaining.astype(jnp.bfloat16).astype(jnp.float32)
            pieces = jnp.where(sublane == index, piece, pieces)
            remaining = remaining - piece
        pair_sum = jnp.sum(
            jnp.dot(
                pieces.astype(jnp.bfloat16), same_query, preferred_element_type=jnp.float32
            ),
            axis=0, keepdims=True,
        )
        pair_score = pair_sum / count_row
        label_row = jnp.zeros((1, block_rows), jnp.float32)
        for index in range(block_queries):
            label = label_ref[0, origin * block_queries + index].astype(jnp.float32)
            label_row = jnp.where(query_row == index, label, label_row)
        label_sign = 2.0 * label_row - 1.0
        signed = -label_sign * (logit_scale * pair_score + logit_bias)
        decay = jnp.exp(-jnp.abs(signed))
        softplus = jnp.maximum(signed, 0.0) + jnp.log1p(decay)
        sigmoid = jnp.where(signed >= 0.0, 1.0, decay) / (1.0 + decay)
        loss_row = jnp.where(token_row == 0, softplus, 0.0)
        token_grad = jnp.where(live, -label_sign * logit_scale * sigmoid / count_row, 0.0) / total
        slope = token_grad * align_sharpness
        offset = token_grad * (1.0 - align_sharpness * shifted_score)
        for tile in tiles:
            tile_grad = exponents[tile, :] * (offset + slope * scores[tile, :])
            grads[origin, tile, :] = tile_grad.astype(jnp.bfloat16)
        query_term = lax.dot_general(
            grads[origin], page_ref[...], (((0,), (0,)), ((), ())),
            preferred_element_type=jnp.float32,
        )
        return query_term, loss_row

    own, loss_row = block_terms(blk)
    own_term[...] = own.reshape(groups, rows, width)

    for step in range(blocks - 1, 0, -1):
        origin = source(blk, step, blocks)
        settle(held.at[origin], row_recv.at[origin])
        settle(count_rows.at[origin], count_recv.at[origin])
        query_term, loss_term = block_terms(origin)
        loss_row = loss_row + loss_term
        part_send[origin] = query_term.astype(jnp.bfloat16).reshape(groups, rows, width)
        remote(
            part_send.at[origin], part_recv.at[blk], part_send_sem, part_recv_sem.at[blk],
            (origin, grp),
        )

    def page_term(tile):
        result = jnp.dot(
            grads[0, tile, :], held[0].reshape(block_rows, width), preferred_element_type=jnp.float32
        )
        for index in range(1, blocks):
            result = result + jnp.dot(
                grads[index, tile, :], held[index].reshape(block_rows, width),
                preferred_element_type=jnp.float32,
            )
        page_grad_ref[tile, :] = result

    half = len(tiles) // 2
    for tile in tiles[:half]:
        page_term(tile)

    block_sum = own_term[...]
    for step in range(blocks - 1, 0, -1):
        origin = source(blk, step, blocks)
        settle(part_recv.at[origin], part_recv_sem.at[origin])
        block_sum = block_sum + part_recv[origin].astype(jnp.float32)
    own_term[...] = block_sum
    sum_send[...] = block_sum.astype(jnp.bfloat16)
    for step in range(groups - 1, 0, -1):
        target = partner(grp, step, groups)
        remote(
            sum_send.at[target], sum_recv.at[step - 1], sum_send_sem, sum_recv_sem, (blk, target)
        )
    for tile in tiles[half:]:
        page_term(tile)
    loss_ref[0] = jnp.sum(loss_row) / jnp.float32(total_queries)

    settle(sum_recv, sum_recv_sem)
    result = own_term[grp]
    for step in range(1, groups):
        result = result + sum_recv[step - 1].astype(jnp.float32)
    query_grad_ref[...] = result

    settle(held.at[0, pl.ds(0, groups - 1)], column_send)
    settle(held.at[pl.ds(0, blocks - 1)], row_send)
    settle(count_rows.at[pl.ds(0, blocks - 1)], count_send)
    settle(part_send.at[pl.ds(0, blocks - 1)], part_send_sem)
    settle(sum_send.at[pl.ds(0, groups - 1)], sum_send_sem)


def write_out(query_grad_in, page_grad_in, loss_in, query_grad_ref, page_grad_ref, loss_ref, sems):
    copies = [
        pltpu.make_async_copy(page_grad_in, page_grad_ref, sems.at[0]),
        pltpu.make_async_copy(query_grad_in, query_grad_ref, sems.at[1]),
        pltpu.make_async_copy(loss_in, loss_ref, sems.at[2]),
    ]
    for copy in copies:
        copy.start()
    for copy in copies:
        copy.wait()


def local(queries, token_counts, pages, patch_counts, labels):
    blocks = lax.axis_size("blk")
    groups = lax.axis_size("grp")
    block_queries, slice_tokens, width = queries.shape
    patches = pages.shape[1]
    rows = block_queries * slice_tokens
    block_rows = rows * groups
    vmem = pl.BlockSpec(memory_space=pltpu.VMEM)
    smem = pl.BlockSpec(memory_space=pltpu.SMEM)
    anywhere = pl.BlockSpec(memory_space=pl.ANY)
    dma = pltpu.SemaphoreType.DMA
    query_grad, page_grad, page_loss = pl.pallas_call(
        functools.partial(kernel, blocks, groups, block_queries, slice_tokens),
        out_shape=(
            pltpu.VMEM((rows, width), jnp.float32),
            pltpu.VMEM((patches, width), jnp.float32),
            pltpu.SMEM((1,), jnp.float32),
        ),
        in_specs=[anywhere] * 5,
        out_specs=(vmem, vmem, smem),
        scratch_shapes=[
            pltpu.VMEM((rows, width), jnp.bfloat16),
            pltpu.SMEM(token_counts.shape, jnp.int32),
            pltpu.VMEM((patches, width), jnp.bfloat16),
            pltpu.SMEM((1,), jnp.int32),
            pltpu.SMEM((1, labels.shape[0]), jnp.int32),
            pltpu.VMEM((blocks, groups, rows, width), jnp.bfloat16),
            pltpu.VMEM((blocks, 1, block_rows), jnp.float32),
            pltpu.VMEM((patches, width), jnp.float32),
            pltpu.VMEM((patches, block_rows), jnp.float32),
            pltpu.VMEM((patches, block_rows), jnp.float32),
            pltpu.VMEM((blocks, patches, block_rows), jnp.bfloat16),
            pltpu.VMEM((groups, rows, width), jnp.float32),
            pltpu.VMEM((blocks, groups, rows, width), jnp.bfloat16),
            pltpu.VMEM((blocks, groups, rows, width), jnp.bfloat16),
            pltpu.VMEM((groups, rows, width), jnp.bfloat16),
            pltpu.VMEM((groups - 1, rows, width), jnp.bfloat16),
            dma, dma((groups,)), dma, dma((blocks,)), dma, dma((blocks,)),
            dma, dma((blocks,)), dma, dma, dma((5,)),
        ],
        compiler_params=pltpu.CompilerParams(
            collective_id=0, has_side_effects=True, vmem_limit_bytes=60 * 1024 * 1024
        ),
        name="late_interaction",
    )(queries.reshape(rows, width), token_counts, pages[0], patch_counts, labels.T)
    query_grad, page_grad, page_loss = pl.pallas_call(
        write_out,
        out_shape=(
            jax.ShapeDtypeStruct((rows, width), jnp.float32),
            jax.ShapeDtypeStruct((patches, width), jnp.float32),
            jax.ShapeDtypeStruct((1,), jnp.float32),
        ),
        in_specs=[anywhere] * 3,
        out_specs=(anywhere,) * 3,
        scratch_shapes=[dma((3,))],
        compiler_params=pltpu.CompilerParams(vmem_limit_bytes=1024 * 1024),
        name="write_out",
    )(query_grad, page_grad, page_loss)
    return query_grad.reshape(queries.shape), page_grad[None], page_loss


def solution(mesh):
    in_specs = (
        P("blk", "grp", None),
        P("blk"),
        P(("blk", "grp"), None, None),
        P(("blk", "grp")),
        P(None, ("blk", "grp")),
    )
    out_specs = (P("blk", "grp", None), P(("blk", "grp"), None, None), P(("blk", "grp")))
    return jax.shard_map(local, mesh=mesh, in_specs=in_specs, out_specs=out_specs, check_vma=False)
```
